32 devices in a mesh: ctx: 8 (over z, x), tp: 4 (over y, core).
Axes of the slice: x: 2, y: 2, z: 4, core: 2. Of those that a mesh axis runs over, the one named last changes fastest.
Arguments:
- queries: bfloat16 [4096, 2048], P('ctx', 'tp'), may hold values from -40 to 40
- keys: bfloat16 [4096, 2048], P('ctx', 'tp'), may hold values from -40 to 40
- values: bfloat16 [4096, 2048], P('ctx', 'tp'), may hold values from -6 to 6
- out_weight: bfloat16 [2048, 4096], P('tp'), may hold values from -0.1875 to 0.1875
- doc_lengths: int32 [16], replicated, may hold values from 1 to 2048, 4096 in all
- layout: int32 [16], replicated, may hold values from 0 to 15, each once
Outputs:
- mixed: bfloat16 [4096, 4096], P('ctx', 'tp')
- log_totals: float32 [16, 4096], P('tp', 'ctx')
The draws below stay inside these ranges and needn't reach their ends.
Inputs may be any that keep to these rules, and one draw needn't show every extreme that they name: `layout`: every block number appears once. `doc_lengths`: the lengths sum to 4096; the longest is exactly 2048.
All inputs are finite; a program needn't handle non-finite values.
Results may differ from the reference program's by a relative error of at most 0.012.
Values may be sent and summed in bfloat16 or wider, within the bound.
No kernel may reach another device: no remote copies, remote signals or barrier semaphores. Data moves between devices by JAX's collectives and lax.ppermute only.
A program may use at most 192 MiB of HBM per device.

```python
import math
import jax
import jax.numpy as jnp
import numpy as np
from jax import lax

D = 4096
HEAD_DIM = 128
HEADS = 16
HALF = 256
SEQ = 4096
BLOCKS = 16
DOCS = 16
LONGEST = 2048


def paired_rows(key):
    shape = (SEQ, HEADS * HEAD_DIM)
    key_part = jax.random.normal(jax.random.fold_in(key, 11), shape, jnp.float32)
    query_part = jax.random.normal(jax.random.fold_in(key, 12), shape, jnp.float32)
    return (jnp.clip(query_part, -40.0, 40.0), jnp.clip(key_part, -40.0, 40.0))


def draw_queries(key, part):
    return paired_rows(key)[0].astype(jnp.bfloat16)


def draw_keys(key, part):
    return paired_rows(key)[1].astype(jnp.bfloat16)


def spiked(entries, stream_key, source, target, parts, factor):
    owner, partner = [(jnp.arange(entries.shape[dim]) // (entries.shape[dim] // parts)).reshape([-1 if axis == dim else 1 for axis in range(entries.ndim)]) for dim in (source, target)]
    chosen = jax.random.permutation(stream_key, parts)[partner]
    strong = (owner == chosen) | (owner == (partner + parts // 2) % parts)
    return jnp.where(strong, factor * entries, entries)


def steps_of(rng, extent, cuts, smallest, high):
    factor_of = 1.0
    for dim, parts in cuts:
        heights = jax.random.uniform(jax.random.fold_in(jax.random.fold_in(rng, 6), dim), (parts,), jnp.float32, smallest / len(cuts), high / len(cuts))
        factor_of = factor_of * jnp.repeat(jnp.exp(heights), extent[dim] // parts).reshape((-1,) + (1,) * (len(extent) - 1 - dim))
    return factor_of


def length_profile(amount, total, bound, skew):
    loads = [(1 << 20) // math.isqrt(standing ** skew) + 1 for standing in range(2, amount + 1)]
    surplus, counts = total - bound - (amount - 1), [1] * (amount - 1)
    while surplus > 0:
        movable = [i for i in range(amount - 1) if counts[i] < bound]
        mass, remaining = sum([loads[i] for i in movable]), surplus
        for i in movable:
            more = min(bound - counts[i], max(1, remaining * loads[i] // mass), surplus)
            counts[i] = counts[i] + more
            surplus = surplus - more
    return np.array([bound] + counts)


def ragged_sizes(key, count, total, most, lean):
    if count == 2:
        one = jax.random.randint(key, (), max(1, total - most), min(most, total - 1) + 1)
        return jnp.stack([one, total - one])
    sizes = jnp.asarray(length_profile(count, total, most, lean), jnp.int32)
    couples = (count - 1) // 2
    giver, sink = sizes[1:1 + 2 * couples:2], sizes[2:2 + 2 * couples:2]
    room = jnp.minimum(giver - 1, most - sink)
    moved = jax.random.randint(jax.random.fold_in(key, 1), (couples,), 0, 1 << 20) % (room + 1)
    sizes = sizes.at[1:1 + 2 * couples:2].set(giver - moved).at[2:2 + 2 * couples:2].set(sink + moved)
    return sizes[jax.random.permutation(jax.random.fold_in(key, 2), count)]


def noise(rng, shape, width, limit, cuts=(), kind=jnp.bfloat16):
    values = jax.random.normal(rng, shape, jnp.float32) * width
    if len(cuts) > 0:
        values = steps_of(rng, shape, cuts, -0.22, 0.18) * values
    return jnp.clip(values, min=-limit, max=limit).astype(kind)


def noise_with(own_key, shape, width, limit, pieces, heavy, held_as=jnp.bfloat16):
    array = width * jax.random.normal(own_key, shape, jnp.float32)
    if pieces:
        array = array * steps_of(own_key, shape, pieces, -0.22, 0.18)
    return jnp.clip(spiked(array, jax.random.fold_in(own_key, 3), *heavy), -limit, limit).astype(held_as)


def setup_inputs(seed: int = 0) -> dict:
    key_list = jax.random.split(jax.random.key(seed), 7)
    return {
        "queries": draw_queries(jax.random.fold_in(key_list[6], 71), 0),
        "keys": draw_keys(jax.random.fold_in(key_list[6], 71), 0),
        "values": noise(key_list[2], (SEQ, HEADS * HEAD_DIM), 1.0, 6.0, ((0, 8), (1, 4))),
        "out_weight": noise_with(key_list[3], (HEADS * HEAD_DIM, D), (HEADS * HEAD_DIM) ** -0.5, 0.1875, ((0, 4),), (0, 1, 4, 2.0)),
        "doc_lengths": ragged_sizes(key_list[4], DOCS, SEQ, LONGEST, 2).astype(jnp.int32),
        "layout": jax.random.permutation(key_list[5], BLOCKS).astype(jnp.int32),
    }


def reference(queries, keys, values, out_weight, doc_lengths, layout):
    seq = queries.shape[0]
    rows = jnp.arange(seq, dtype=jnp.int32)
    position = (layout[rows // HALF] * HALF + rows % HALF).astype(jnp.int32)
    starts = (jnp.cumsum(doc_lengths) - doc_lengths).astype(jnp.int32)
    document = (jnp.sum((starts[None, :] <= position[:, None]).astype(jnp.int32), axis=1) - 1).astype(jnp.int32)
    key_all = keys.astype(jnp.float32).reshape(seq, HEADS, HEAD_DIM)
    value_all = values.astype(jnp.float32).reshape(seq, HEADS, HEAD_DIM)
    blk = min(512, seq)
    scale = 1.0 / (HEAD_DIM ** 0.5)

    def one_block(index):
        first = (index * blk).astype(jnp.int32)
        query_blk = lax.dynamic_slice_in_dim(queries, first, blk, 0).astype(jnp.float32).reshape(blk, HEADS, HEAD_DIM)
        query_pos = lax.dynamic_slice_in_dim(position, first, blk, 0)
        query_doc = lax.dynamic_slice_in_dim(document, first, blk, 0)
        scores = jnp.einsum('qhd,khd->hqk', query_blk, key_all) * scale
        allowed = (document[None, :] == query_doc[:, None]) & (position[None, :] <= query_pos[:, None])
        scores = jnp.where(allowed[None], scores, -1e30)
        top = jnp.max(scores, axis=-1)
        weights = jnp.where(allowed[None], jnp.exp(scores - top[..., None]), 0.0)
        totals = jnp.sum(weights, axis=-1)
        summed = jnp.einsum('hqk,khd->qhd', weights.astype(jnp.bfloat16).astype(jnp.float32), value_all)
        attended = (summed / totals.T[:, :, None]).reshape(blk, HEADS * HEAD_DIM).astype(jnp.bfloat16)
        return attended, top + jnp.log(totals)

    attended, logs = lax.map(one_block, jnp.arange(seq // blk, dtype=jnp.int32))
    attended = attended.reshape(seq, HEADS * HEAD_DIM)
    log_totals = jnp.transpose(logs, (1, 0, 2)).reshape(HEADS, seq)
    mixed = jnp.dot(attended, out_weight, preferred_element_type=jnp.float32).astype(jnp.bfloat16)
    return mixed, log_totals
```

```python
import functools
import math

import jax
import jax.numpy as jnp
from jax import lax
from jax.experimental import pallas as pl
from jax.experimental.pallas import tpu as pltpu
from jax.sharding import PartitionSpec as P

HEAD_DIM = 128
NEG = -1e30


HBM_SPEC = pl.BlockSpec(memory_space=pltpu.MemorySpace.HBM)
VMEM_SPEC = pl.BlockSpec(memory_space=pltpu.MemorySpace.VMEM)
SMEM_SPEC = pl.BlockSpec(memory_space=pltpu.MemorySpace.SMEM)


def attention_kernel(places, spread, layout_ref, lens_ref, *refs):
    chunks = places * spread
    q_refs, refs = refs[:places], refs[places:]
    kv_refs, refs = refs[:chunks], refs[chunks:]
    out_refs, refs = refs[:places], refs[places:]
    log_refs, refs = refs[:places], refs[places:]
    k_all, v_all, q_all, sems, q_sems = refs
    rows = q_refs[0].shape[0]
    half = rows // 2
    width = 2 * half
    docs = lens_ref.shape[0]
    me = lax.axis_index("ctx")
    z, r = me // spread, me % spread
    factor = math.log2(math.e) / math.sqrt(HEAD_DIM)

    copies = []
    for s in range(places):
        copy = pltpu.make_async_copy(q_refs[s], q_all.at[pl.ds(s * rows, rows)], q_sems.at[s])
        copy.start()
        copies.append(copy)
    for s in range(places):
        for t in range(spread):
            owner = ((z + places - s) % places) * spread + (r + spread - t) % spread
            for b in range(2):
                first = pl.multiple_of(layout_ref[owner * 2 + b] * half, half)
                for which, buf in ((0, k_all), (1, v_all)):
                    copy = pltpu.make_async_copy(
                        kv_refs[s * spread + t].at[which, pl.ds(b * half, half)],
                        buf.at[pl.ds(first, half)],
                        sems.at[s * spread + t, b, which],
                    )
                    copy.start()
                    copies.append(copy)
    total = layout_ref.shape[0] * half
    v_all[pl.ds(total, half), :] = jnp.zeros((half, HEAD_DIM), v_all.dtype)
    for copy in copies:
        copy.wait()

    for index in range(2 * places):
        s, b = index // 2, index % 2
        owner = ((z + places - s) % places) * spread + r
        block = layout_ref[owner * 2 + b]
        first = block * half

        def scan(j, carry):
            end, low, before, inside = carry
            end_next = end + lens_ref[j]
            low = jnp.where(end <= first, end, low)
            before = before + jnp.where(end <= first, 1, 0)
            inside = inside + jnp.where(end < first + half, 1, 0)
            return end_next, low, before, inside

        zero = jnp.int32(0)
        _, low, before, inside = lax.fori_loop(0, docs, scan, (zero, zero, zero, zero))
        row_pos = first + lax.broadcasted_iota(jnp.int32, (half, 1), 0)

        def bounds(j, carry):
            start, row_start = carry
            start = start + lens_ref[j - 1]
            return start, jnp.where(row_pos >= start, start, row_start)

        _, row_start = lax.fori_loop(
            before, inside, bounds, (low, jnp.full((half, 1), low, jnp.int32))
        )
        low_block = low // half
        query = q_all[pl.ds(index * half, half), :]

        def step(i, carry):
            top, sums, summed = carry
            base = pl.multiple_of((low_block + 2 * i) * half, half)
            scores = lax.dot_general(
                query,
                k_all[pl.ds(base, width), :],
                (((1,), (1,)), ((), ())),
                preferred_element_type=jnp.float32,
            )
            col = base + lax.broadcasted_iota(jnp.int32, (half, width), 1)
            scores = jnp.where((col >= row_start) & (col <= row_pos), scores, NEG)
            new_top = jnp.maximum(top, jnp.max(scores, axis=1, keepdims=True))
            weights = jnp.exp2((scores - new_top) * factor)
            scale = jnp.exp2((top - new_top) * factor)
            sums = sums * scale + jnp.sum(weights, axis=1, keepdims=True)
            summed = summed * scale + jnp.dot(
                weights.astype(jnp.bfloat16),
                v_all[pl.ds(base, width), :],
                preferred_element_type=jnp.float32,
            )
            return new_top, sums, summed

        top, sums, summed = lax.fori_loop(
            0,
            (block - low_block + 2) // 2,
            step,
            (
                jnp.full((half, 1), NEG, jnp.float32),
                jnp.zeros((half, 1), jnp.float32),
                jnp.zeros((half, HEAD_DIM), jnp.float32),
            ),
        )
        out_refs[s][pl.ds(b * half, half), :] = (summed / sums).astype(jnp.bfloat16)
        logs = top * (1.0 / math.sqrt(HEAD_DIM)) + jnp.log(sums)
        log_refs[s][:, pl.ds(b * half, half)] = jnp.broadcast_to(logs, (half, HEAD_DIM)).T[0:1, :]


def attend(layout, doc_lengths, q_parts, kv_parts, places, spread):
    rows = q_parts[0].shape[0]
    half = rows // 2
    total = layout.shape[0] * half
    return pl.pallas_call(
        functools.partial(attention_kernel, places, spread),
        out_shape=[jax.ShapeDtypeStruct((rows, HEAD_DIM), jnp.bfloat16)] * places
        + [jax.ShapeDtypeStruct((1, rows), jnp.float32)] * places,
        in_specs=[SMEM_SPEC] * 2 + [HBM_SPEC] * (places + places * spread),
        out_specs=[VMEM_SPEC] * (2 * places),
        scratch_shapes=[
            pltpu.VMEM((total + half, HEAD_DIM), jnp.bfloat16),
            pltpu.VMEM((total + half, HEAD_DIM), jnp.bfloat16),
            pltpu.VMEM((places * rows, HEAD_DIM), jnp.bfloat16),
            pltpu.SemaphoreType.DMA((places * spread, 2, 2)),
            pltpu.SemaphoreType.DMA((places,)),
        ],
        name="attend",
    )(layout, doc_lengths, *q_parts, *kv_parts)


def project_kernel(places, spread, groups, *refs):
    parts, refs = refs[: groups * places], refs[groups * places :]
    w_refs, refs = refs[:groups], refs[groups:]
    logs, refs = refs[:places], refs[places:]
    out_ref, log_ref, att, weight, part_sems, w_sems = refs
    z = lax.axis_index("ctx") // spread
    copies = []
    for m in range(groups):
        mine = []
        for s in range(places):
            head = (z + s) % places
            mine.append(
                pltpu.make_async_copy(
                    parts[m * places + s],
                    att.at[m, :, pl.ds(pl.multiple_of(head * HEAD_DIM, HEAD_DIM), HEAD_DIM)],
                    part_sems.at[m, s],
                )
            )
        mine.append(pltpu.make_async_copy(w_refs[m], weight.at[m], w_sems.at[m]))
        for copy in mine:
            copy.start()
        copies.append(mine)
    for s in range(places):
        head = (z + s) % places
        log_ref[pl.ds(head, 1), :] = logs[s][...]
    total = None
    for m in range(groups):
        for copy in copies[m]:
            copy.wait()
        part = jnp.dot(att[m], weight[m], preferred_element_type=jnp.float32)
        total = part if total is None else total + part
    out_ref[...] = total.astype(out_ref.dtype)


def project(parts, weights, logs, places, spread):
    groups = len(weights)
    rows = parts[0].shape[0]
    depth, columns = weights[0].shape
    return pl.pallas_call(
        functools.partial(project_kernel, places, spread, groups),
        out_shape=[
            jax.ShapeDtypeStruct((rows, columns), jnp.bfloat16),
            jax.ShapeDtypeStruct((places, rows), jnp.float32),
        ],
        in_specs=[HBM_SPEC] * (len(parts) + groups) + [VMEM_SPEC] * places,
        out_specs=[VMEM_SPEC] * 2,
        scratch_shapes=[
            pltpu.VMEM((groups, rows, depth), jnp.bfloat16),
            pltpu.VMEM((groups, depth, columns), jnp.bfloat16),
            pltpu.SemaphoreType.DMA((groups, places)),
            pltpu.SemaphoreType.DMA((groups,)),
        ],
        name="project",
    )(*parts, *weights, *logs)


def local(ctx, tp, queries, keys, values, out_weight, doc_lengths, layout):
    places = queries.shape[1] // HEAD_DIM
    spread = ctx // places
    me = lax.axis_index("ctx")
    z = me // spread
    tp_me = lax.axis_index("tp")

    def over_places(array, s):
        if s == 0:
            return array
        pairs = [(i, (i // spread + s) % places * spread + i % spread) for i in range(ctx)]
        return lax.ppermute(array, "ctx", pairs)

    def over_spread(array, t):
        if t == 0:
            return array
        pairs = [(i, i // spread * spread + (i % spread + t) % spread) for i in range(ctx)]
        return lax.ppermute(array, "ctx", pairs)

    def over_tp(array, m):
        if m == 0:
            return array
        return lax.ppermute(array, "tp", [(i, i ^ m) for i in range(tp)])

    def head(array, s):
        return lax.dynamic_slice_in_dim(array, (z + s) % places * HEAD_DIM, HEAD_DIM, 1)

    kv_parts = [[None] * spread for _ in range(places)]
    for s in range(places):
        kv_parts[s][0] = over_places(jnp.stack([head(keys, s), head(values, s)]), s)
    q_parts = [over_places(head(queries, s), s) for s in range(places)]
    for s in range(places):
        for t in range(1, spread):
            kv_parts[s][t] = over_spread(kv_parts[s][0], t)

    columns = out_weight.shape[1] // tp
    weights = [
        over_tp(lax.dynamic_slice_in_dim(out_weight, (tp_me ^ m) * columns, columns, 1), m)
        for m in range(tp)
    ]

    results = attend(
        layout, doc_lengths, q_parts, [part for parts in kv_parts for part in parts], places, spread
    )
    heads = [over_places(results[s], -s % places) for s in range(places)]
    logs = [over_places(results[places + s], -s % places) for s in range(places)]

    groups = {0: heads}
    bit = tp // 2
    while bit:
        for m in list(groups):
            groups[m | bit] = [over_tp(part, bit) for part in groups[m]]
        bit //= 2
    parts = [part for m in range(tp) for part in groups[m]]
    return project(parts, weights, logs, places, spread)


def solution(mesh):
    placed = (P("ctx", "tp"), P("ctx", "tp"), P("ctx", "tp"), P("tp", None), P(), P())
    return jax.shard_map(
        functools.partial(local, mesh.shape["ctx"], mesh.shape["tp"]),
        mesh=mesh,
        in_specs=placed,
        out_specs=(P("ctx", "tp"), P("tp", "ctx")),
        check_vma=False,
    )
```

```python
import functools
import math

import jax
import jax.numpy as jnp
from jax import lax
from jax.experimental import pallas as pl
from jax.experimental.pallas import tpu as pltpu
from jax.sharding import PartitionSpec as P

HEAD_DIM = 128
NEG = -1e30
LOG_ROWS = 16
ONES = 16
LONE, LAST = 3, 2
PACK_ORDER = (3, 1, 0, 2)
ATTEND_ORDER = (3, 1, 2, 0)


HBM_SPEC = pl.BlockSpec(memory_space=pltpu.MemorySpace.HBM)
VMEM_SPEC = pl.BlockSpec(memory_space=pltpu.MemorySpace.VMEM)
MIB = 1 << 20
SMEM_SPEC = pl.BlockSpec(memory_space=pltpu.MemorySpace.SMEM)


def pack_kernel(places, spread, k_ref, v_ref, q_ref, *refs):
    kv_out, q_out, (v_rows, sems) = refs[:places], refs[places : 2 * places], refs[2 * places :]
    z = lax.axis_index("ctx") // spread
    rows = k_ref.shape[0]
    copies = []
    for s in PACK_ORDER:
        columns = pl.ds(pl.multiple_of((z ^ s) * HEAD_DIM, HEAD_DIM), HEAD_DIM)
        copies.append(
            [
                pltpu.make_async_copy(v_ref.at[:, columns], v_rows.at[s], sems.at[s, 0]),
                pltpu.make_async_copy(k_ref.at[:, columns], kv_out[s].at[0], sems.at[s, 1]),
                pltpu.make_async_copy(q_ref.at[:, columns], q_out[s], sems.at[s, 2]),
            ]
        )
    for group in copies:
        for copy in group:
            copy.start()
    for s, group in zip(PACK_ORDER, copies):
        group[0].wait()
        for i in range(0, rows, HEAD_DIM):
            kv_out[s][1, i : i + HEAD_DIM, :] = v_rows[s, i : i + HEAD_DIM, :].T
    for group in copies:
        group[1].wait()
        group[2].wait()


def pack(keys, values, queries, places, spread):
    rows = keys.shape[0]
    return pl.pallas_call(
        functools.partial(pack_kernel, places, spread),
        out_shape=[jax.ShapeDtypeStruct((2, rows, HEAD_DIM), keys.dtype)] * places
        + [jax.ShapeDtypeStruct((rows, HEAD_DIM), keys.dtype)] * places,
        in_specs=[HBM_SPEC] * 3,
        out_specs=[VMEM_SPEC] * (2 * places),
        scratch_shapes=[
            pltpu.VMEM((places, rows, HEAD_DIM), keys.dtype),
            pltpu.SemaphoreType.DMA((places, 3)),
        ],
        compiler_params=pltpu.CompilerParams(vmem_limit_bytes=8 * MIB),
        name="pack",
    )(*(pltpu.with_memory_space_constraint(x, pltpu.HBM) for x in (keys, values, queries)))


def plan_kernel(places, spread, half, layout_ref, lens_ref, table_ref, bounds_ref):
    me = lax.axis_index("ctx")
    z, r = me // spread, me % spread
    count = 2 * places
    blocks = [layout_ref[((z ^ (i // 2)) * spread + r) * 2 + i % 2] for i in range(count)]
    index = lax.broadcasted_iota(jnp.int32, (count, half), 0)
    row_pos = lax.broadcasted_iota(jnp.int32, (count, half), 1)
    for i, block in enumerate(blocks):
        row_pos = row_pos + jnp.where(index == i, block * half, 0)

    def scan(j, carry):
        end, row_start, *lows = carry
        lows = [jnp.where(end <= block * half, end, low) for block, low in zip(blocks, lows)]
        row_start = jnp.where(row_pos >= end, end, row_start)
        return end + lens_ref[j], row_start, *lows

    zero = jnp.int32(0)
    _, row_start, *lows = lax.fori_loop(
        0, lens_ref.shape[0], scan, (zero, jnp.zeros((count, half), jnp.int32), *([zero] * count))
    )
    for i in range(count):
        table_ref[2 * i] = blocks[i]
        table_ref[2 * i + 1] = lows[i] // half
    bounds_ref[:count, :] = row_start
    bounds_ref[count:, :] = row_pos - row_start


def plan(layout, doc_lengths, places, spread, half):
    return pl.pallas_call(
        functools.partial(plan_kernel, places, spread, half),
        out_shape=[
            jax.ShapeDtypeStruct((4 * places,), jnp.int32),
            jax.ShapeDtypeStruct((4 * places, half), jnp.int32),
        ],
        in_specs=[SMEM_SPEC] * 2,
        out_specs=[SMEM_SPEC, VMEM_SPEC],
        compiler_params=pltpu.CompilerParams(vmem_limit_bytes=2 * MIB),
        name="plan",
    )(layout, doc_lengths)


def pack_weight_kernel(tp, columns, w_ref, *refs):
    outs, sems = refs[:-1], refs[-1]
    me, side = lax.axis_index("tp"), lax.axis_index("ctx") % 2
    copies = []
    for m in range(tp):
        depth = outs[m].shape[0]
        first = 0 if depth == w_ref.shape[0] else pl.multiple_of(side * depth, depth)
        copies.append(
            pltpu.make_async_copy(
                w_ref.at[
                    pl.ds(first, depth), pl.ds(pl.multiple_of((me ^ m) * columns, columns), columns)
                ],
                outs[m],
                sems.at[m],
            )
        )
    for copy in copies:
        copy.start()
    for copy in copies:
        copy.wait()


def pack_weight(weight, tp):
    depth, columns = weight.shape[0], weight.shape[1] // tp
    return pl.pallas_call(
        functools.partial(pack_weight_kernel, tp, columns),
        out_shape=[
            jax.ShapeDtypeStruct((depth // (1 if m < tp - 1 else 2), columns), weight.dtype)
            for m in range(tp)
        ],
        in_specs=[HBM_SPEC],
        out_specs=[VMEM_SPEC] * tp,
        scratch_shapes=[pltpu.SemaphoreType.DMA((tp,))],
        compiler_params=pltpu.CompilerParams(vmem_limit_bytes=8 * MIB),
        name="pack_weight",
    )(pltpu.with_memory_space_constraint(weight, pltpu.HBM))


def attention_kernel(place, places, spread, layout_ref, table_ref, bounds_ref, q_ref, *refs):
    refs, (scores, peaks, tops, summed) = refs[:-4], refs[-4:]
    sort = len(refs) != 3
    if sort:
        kv_refs, (out_ref, k_all, v_all) = refs[:-3], refs[-3:]
    else:
        k_all, v_all, out_ref = refs
    rows = q_ref.shape[0]
    half = rows // 2
    width = 2 * half
    factor = math.log2(math.e) / math.sqrt(HEAD_DIM)

    if sort:
        me = lax.axis_index("ctx")
        z, r = me // spread, me % spread
        for s in range(places):
            for t in range(spread):
                owner = (z ^ s) * spread + (r + spread - t) % spread
                chunk = kv_refs[s * spread + t]
                for b in range(2):
                    first = pl.multiple_of(layout_ref[owner * 2 + b] * half, half)
                    k_all[pl.ds(first, half), :] = chunk[0, b * half : (b + 1) * half, :]
                    for i in range(0, half, HEAD_DIM):
                        columns = pl.ds(pl.multiple_of(first + i, HEAD_DIM), HEAD_DIM)
                        v_all[:HEAD_DIM, columns] = chunk[
                            1, b * half + i : b * half + i + HEAD_DIM, :
                        ]
        total = layout_ref.shape[0] * half
        k_all[total:, :] = jnp.zeros((half, HEAD_DIM), k_all.dtype)
        v_all[:HEAD_DIM, total:] = jnp.zeros((HEAD_DIM, half), v_all.dtype)
        v_all[HEAD_DIM:, :] = jnp.ones((ONES, total + half), v_all.dtype)

    blocks = [table_ref[4 * place + 2 * b] for b in range(2)]
    lows = [table_ref[4 * place + 2 * b + 1] for b in range(2)]
    counts = [(blocks[b] - lows[b] + 2) // 2 for b in range(2)]
    items = counts[0] + counts[1]
    key_row = lax.broadcasted_iota(jnp.int32, (width, half), 0)
    tops[...] = jnp.full(tops.shape, NEG, jnp.float32)
    summed[...] = jnp.zeros(summed.shape, jnp.float32)

    def where_of(item):
        late = jnp.logical_and(item >= counts[0], item < items).astype(jnp.int32)
        low = jnp.where(late == 1, lows[1], lows[0])
        step = jnp.where(item < items, item - late * counts[0], 0)
        base = pl.multiple_of((low + 2 * step) * half, half)
        return late, base

    def score(item, slot):
        late, base = where_of(item)
        raw = lax.dot_general(
            k_all[pl.ds(base, width), :],
            q_ref[pl.ds(pl.multiple_of(late * half, half), half), :],
            (((1,), (1,)), ((), ())),
            preferred_element_type=jnp.float32,
        )
        row = 2 * place + late
        start = bounds_ref[pl.ds(row, 1), :] - jnp.where(item < items, base, -(1 << 30))
        span = bounds_ref[pl.ds(2 * places + row, 1), :].astype(jnp.uint32)
        masked = jnp.where((key_row - start).astype(jnp.uint32) <= span, raw, NEG)
        scores[slot] = masked
        peaks[slot] = jnp.max(masked, axis=0, keepdims=True)

    def absorb(item, slot):
        late, base = where_of(item)
        top = tops[late]
        new_top = jnp.maximum(top, peaks[slot])
        weights = jnp.exp2((scores[slot] - new_top) * factor)
        scale = jnp.exp2((top - new_top) * factor)
        tops[late] = new_top
        summed[late] = summed[late] * scale + jnp.dot(
            v_all[:, pl.ds(base, width)],
            weights.astype(jnp.bfloat16),
            preferred_element_type=jnp.float32,
        )

    score(0, 0)

    def pair(i, carry):
        score(2 * i + 1, 1)
        absorb(2 * i, 0)
        score(2 * i + 2, 0)
        absorb(2 * i + 1, 1)
        return carry

    lax.fori_loop(0, (items + 1) // 2, pair, 0)

    log_rows = []
    for b in range(2):
        sums = summed[b, HEAD_DIM : HEAD_DIM + 1, :]
        mean = summed[b, :HEAD_DIM, :] / sums
        out_ref[b * half : (b + 1) * half, :] = mean.T.astype(jnp.bfloat16)
        logs = tops[b] * (1.0 / math.sqrt(HEAD_DIM)) + jnp.log(sums)
        log_rows += [logs[:, i : i + HEAD_DIM] for i in range(0, half, HEAD_DIM)]
    left = jnp.concatenate(log_rows, axis=0)
    split = []
    for _ in range(3):
        piece = left.astype(jnp.bfloat16).astype(jnp.float32)
        split.append(piece)
        left = left - piece
    split.append(jnp.zeros((LOG_ROWS - 3 * len(log_rows), HEAD_DIM), jnp.float32))
    out_ref[pl.ds(rows, LOG_ROWS), :] = jnp.concatenate(split, axis=0).astype(jnp.bfloat16)


def attend(layout, table, bounds, query, sources, place, places, spread):
    rows = query.shape[0]
    half = rows // 2
    total = layout.shape[0] * half
    first = len(sources) != 2
    out_shape = [jax.ShapeDtypeStruct((rows + LOG_ROWS, HEAD_DIM), jnp.bfloat16)]
    if first:
        out_shape += [
            jax.ShapeDtypeStruct((total + half, HEAD_DIM), jnp.bfloat16),
            jax.ShapeDtypeStruct((HEAD_DIM + ONES, total + half), jnp.bfloat16),
        ]
    return pl.pallas_call(
        functools.partial(attention_kernel, place, places, spread),
        out_shape=out_shape,
        in_specs=[SMEM_SPEC] * 2 + [VMEM_SPEC] * (2 + len(sources)),
        out_specs=[VMEM_SPEC] * len(out_shape),
        scratch_shapes=[
            pltpu.VMEM((2, 2 * half, half), jnp.float32),
            pltpu.VMEM((2, 1, half), jnp.float32),
            pltpu.VMEM((2, 1, half), jnp.float32),
            pltpu.VMEM((2, HEAD_DIM + ONES, half), jnp.float32),
        ],
        compiler_params=pltpu.CompilerParams(vmem_limit_bytes=24 * MIB),
    )(layout, table, bounds, query, *sources)


def weight_rows(w_refs, m, z, side, s, pair):
    head = z ^ s
    count = 2 * HEAD_DIM if pair else HEAD_DIM
    if m < len(w_refs) - 2:
        first = (head // 2) * 2 if pair else head
        return w_refs[m][pl.ds(pl.multiple_of(first * HEAD_DIM, count), count), :]
    rows = pl.ds(0 if pair else pl.multiple_of((head % 2) * HEAD_DIM, HEAD_DIM), count)
    near, far = w_refs[-2:]
    return jnp.where(head // 2 == side, near[rows, :], far[rows, :])


def lone_terms(parts, w_refs, tp, z, side, s):
    total = None
    for m in range(0, tp, 2):
        left = jnp.concatenate([parts[m], parts[m + 1]], axis=1)
        right = jnp.concatenate(
            [weight_rows(w_refs, m + i, z, side, s, False) for i in range(2)], axis=0
        )
        term = jnp.dot(left, right, preferred_element_type=jnp.float32)
        total = term if total is None else total + term
    return total


def early_kernel(spread, tp, *refs):
    parts, w_refs, out_ref = refs[: 3 * tp], refs[3 * tp : -1], refs[-1]
    rows = out_ref.shape[0]
    me = lax.axis_index("ctx")
    z, side = me // spread, me % 2
    total = lone_terms([parts[2 * tp + m][:rows, :] for m in range(tp)], w_refs, tp, z, side, LONE)
    turn = z % 2 == 1
    for m in range(tp):
        here, there = parts[m][:rows, :], parts[tp + m][:rows, :]
        left = jnp.concatenate(
            [jnp.where(turn, there, here), jnp.where(turn, here, there)], axis=1
        )
        right = weight_rows(w_refs, m, z, side, 0, True)
        total = total + jnp.dot(left, right, preferred_element_type=jnp.float32)
    out_ref[...] = total


def late_kernel(places, spread, tp, *refs):
    parts, logs_in, w_refs = refs[:tp], refs[tp : tp + places - 1], refs[tp + places - 1 : -3]
    early_ref, out_ref, log_ref = refs[-3:]
    rows = out_ref.shape[0]
    me = lax.axis_index("ctx")
    z, side = me // spread, me % 2
    term = lone_terms([part[:rows, :] for part in parts], w_refs, tp, z, side, LAST)
    out_ref[...] = (early_ref[...] + term).astype(out_ref.dtype)
    count = rows // HEAD_DIM
    logs = {}
    for s, part in zip((0, 1, LONE, LAST), (*logs_in, parts[0])):
        tail = part[pl.ds(rows, LOG_ROWS), :].astype(jnp.float32)
        logs[s] = tail[:count] + tail[count : 2 * count] + tail[2 * count : 3 * count]
    for head in range(places):
        mine = logs[0]
        for s in range(1, places):
            mine = jnp.where(z ^ s == head, logs[s], mine)
        for i in range(count):
            log_ref[head : head + 1, i * HEAD_DIM : (i + 1) * HEAD_DIM] = mine[i : i + 1, :]


def project(groups, weights, places, spread, tp):
    rows = groups[0][0].shape[0] - LOG_ROWS
    columns = weights[0].shape[1]
    params = pltpu.CompilerParams(vmem_limit_bytes=16 * MIB)
    early_parts = [groups[m][s] for s in (0, 1, LONE) for m in range(tp)]
    early = pl.pallas_call(
        functools.partial(early_kernel, spread, tp),
        out_shape=jax.ShapeDtypeStruct((rows, columns), jnp.float32),
        in_specs=[VMEM_SPEC] * (len(early_parts) + len(weights)),
        out_specs=VMEM_SPEC,
        compiler_params=params,
        name="early",
    )(*early_parts, *weights)
    late_parts = [groups[m][LAST] for m in range(tp)] + [groups[0][s] for s in (0, 1, LONE)]
    return pl.pallas_call(
        functools.partial(late_kernel, places, spread, tp),
        out_shape=[
            jax.ShapeDtypeStruct((rows, columns), jnp.bfloat16),
            jax.ShapeDtypeStruct((places, rows), jnp.float32),
        ],
        in_specs=[VMEM_SPEC] * (len(late_parts) + len(weights) + 1),
        out_specs=[VMEM_SPEC] * 2,
        compiler_params=params,
        name="late",
    )(*late_parts, *weights, early)


def local(ctx, tp, queries, keys, values, out_weight, doc_lengths, layout):
    places = queries.shape[1] // HEAD_DIM
    spread = ctx // places
    assert places == 4 and tp == 4 and spread % 2 == 0

    def move(array, axis, target):
        count = ctx if axis == "ctx" else tp
        return lax.ppermute(array, axis, [(i, target(i)) for i in range(count)])

    def over_places(array, s):
        return move(array, "ctx", lambda i: ((i // spread) ^ s) * spread + i % spread)

    def over_spread(array, t):
        return move(array, "ctx", lambda i: i // spread * spread + (i % spread + t) % spread)

    def over_tp(array, m):
        return move(array, "tp", lambda i: i ^ m)

    packed = pack(keys, values, queries, places, spread)
    kv, q = packed[:places], packed[places:]
    q = [q[0]] + [over_places(q[s], s) for s in range(1, places)]
    sources = []
    for s in range(places):
        sources.append(over_places(kv[s], s) if s else kv[0])
        sources += [over_spread(sources[-1], t) for t in range(1, spread)]

    packed_weight = pack_weight(out_weight, tp)
    weights = [packed_weight[0]] + [over_tp(packed_weight[m], m) for m in range(1, tp)]
    weights.append(move(weights[-1], "ctx", lambda i: i ^ 1))

    table, bounds = plan(layout, doc_lengths, places, spread, keys.shape[0] // 2)
    heads = [None] * places
    for s in ATTEND_ORDER:
        message, *rest = attend(layout, table, bounds, q[s], sources, s, places, spread)
        sources = rest or sources
        heads[s] = over_places(message, s) if s else message

    groups = [heads]
    groups.append([over_tp(heads[s], 1) for s in range(places)])
    groups.append([over_tp(heads[s], 2) for s in range(places)])
    groups.append([over_tp(groups[2][s], 1) for s in range(places)])
    return project(groups, weights, places, spread, tp)


def solution(mesh):
    placed = (P("ctx", "tp"), P("ctx", "tp"), P("ctx", "tp"), P("tp", None), P(), P())
    return jax.shard_map(
        functools.partial(local, mesh.shape["ctx"], mesh.shape["tp"]),
        mesh=mesh,
        in_specs=placed,
        out_specs=(P("ctx", "tp"), P("tp", "ctx")),
        check_vma=False,
    )
```

```python
import functools
import math

import jax
import jax.numpy as jnp
from jax import lax
from jax.experimental import pallas as pl
from jax.experimental.pallas import tpu as pltpu
from jax.sharding import PartitionSpec as P

HEAD_DIM = 128
NEG = -1e30
LOG_ROWS = 16
ONES = 16
UNROLL = 4
AHEAD = 3
SLOTS = 4
LONE, LAST = 3, 2
PACK_ORDER = (3, 1, 0, 2)
ATTEND_ORDER = (0, 3, 1, 2)


HBM_SPEC = pl.BlockSpec(memory_space=pltpu.MemorySpace.HBM)
VMEM_SPEC = pl.BlockSpec(memory_space=pltpu.MemorySpace.VMEM)
MIB = 1 << 20
SMEM_SPEC = pl.BlockSpec(memory_space=pltpu.MemorySpace.SMEM)


def pack_kernel(places, spread, k_ref, v_ref, q_ref, *refs):
    kv_out, q_out, (v_rows, sems) = refs[:places], refs[places : 2 * places], refs[2 * places :]
    z = lax.axis_index("ctx") // spread
    rows = k_ref.shape[0]
    copies = []
    for s in PACK_ORDER:
        columns = pl.ds(pl.multiple_of((z ^ s) * HEAD_DIM, HEAD_DIM), HEAD_DIM)
        copies.append(
            [
                pltpu.make_async_copy(v_ref.at[:, columns], v_rows.at[s], sems.at[s, 0]),
                pltpu.make_async_copy(k_ref.at[:, columns], kv_out[s].at[0], sems.at[s, 1]),
                pltpu.make_async_copy(q_ref.at[:, columns], q_out[s], sems.at[s, 2]),
            ]
        )
    for group in copies:
        for copy in group:
            copy.start()
    for s, group in zip(PACK_ORDER, copies):
        group[0].wait()
        for i in range(0, rows, HEAD_DIM):
            kv_out[s][1, i : i + HEAD_DIM, :] = v_rows[s, i : i + HEAD_DIM, :].T
    for group in copies:
        group[1].wait()
        group[2].wait()


def pack(keys, values, queries, places, spread):
    rows = keys.shape[0]
    return pl.pallas_call(
        functools.partial(pack_kernel, places, spread),
        out_shape=[jax.ShapeDtypeStruct((2, rows, HEAD_DIM), keys.dtype)] * places
        + [jax.ShapeDtypeStruct((rows, HEAD_DIM), keys.dtype)] * places,
        in_specs=[HBM_SPEC] * 3,
        out_specs=[VMEM_SPEC] * (2 * places),
        scratch_shapes=[
            pltpu.VMEM((places, rows, HEAD_DIM), keys.dtype),
            pltpu.SemaphoreType.DMA((places, 3)),
        ],
        compiler_params=pltpu.CompilerParams(vmem_limit_bytes=8 * MIB),
        name="pack",
    )(*(pltpu.with_memory_space_constraint(x, pltpu.HBM) for x in (keys, values, queries)))


def plan_kernel(places, spread, half, layout_ref, lens_ref, table_ref, bounds_ref):
    me = lax.axis_index("ctx")
    z, r = me // spread, me % spread
    count = 2 * places
    blocks = [layout_ref[((z ^ (i // 2)) * spread + r) * 2 + i % 2] for i in range(count)]
    index = lax.broadcasted_iota(jnp.int32, (count, half), 0)
    row_pos = lax.broadcasted_iota(jnp.int32, (count, half), 1)
    for i, block in enumerate(blocks):
        row_pos = row_pos + jnp.where(index == i, block * half, 0)

    def scan(j, carry):
        end, row_start, *lows = carry
        lows = [jnp.where(end <= block * half, end, low) for block, low in zip(blocks, lows)]
        row_start = jnp.where(row_pos >= end, end, row_start)
        return end + lens_ref[j], row_start, *lows

    zero = jnp.int32(0)
    _, row_start, *lows = lax.fori_loop(
        0, lens_ref.shape[0], scan, (zero, jnp.zeros((count, half), jnp.int32), *([zero] * count))
    )
    for i in range(count):
        table_ref[2 * i] = blocks[i]
        table_ref[2 * i + 1] = lows[i] // half
    bounds_ref[:count, :] = row_start
    bounds_ref[count:, :] = row_pos - row_start


def plan(layout, doc_lengths, places, spread, half):
    return pl.pallas_call(
        functools.partial(plan_kernel, places, spread, half),
        out_shape=[
            jax.ShapeDtypeStruct((4 * places,), jnp.int32),
            jax.ShapeDtypeStruct((4 * places, half), jnp.int32),
        ],
        in_specs=[SMEM_SPEC] * 2,
        out_specs=[SMEM_SPEC, VMEM_SPEC],
        compiler_params=pltpu.CompilerParams(vmem_limit_bytes=2 * MIB),
        name="plan",
    )(layout, doc_lengths)


def pack_weight_kernel(tp, columns, w_ref, *refs):
    outs, sems = refs[:-1], refs[-1]
    me, side = lax.axis_index("tp"), lax.axis_index("ctx") % 2
    copies = []
    for m in range(tp):
        depth = outs[m].shape[0]
        first = 0 if depth == w_ref.shape[0] else pl.multiple_of(side * depth, depth)
        copies.append(
            pltpu.make_async_copy(
                w_ref.at[
                    pl.ds(first, depth), pl.ds(pl.multiple_of((me ^ m) * columns, columns), columns)
                ],
                outs[m],
                sems.at[m],
            )
        )
    for copy in copies:
        copy.start()
    for copy in copies:
        copy.wait()


def pack_weight(weight, tp):
    depth, columns = weight.shape[0], weight.shape[1] // tp
    return pl.pallas_call(
        functools.partial(pack_weight_kernel, tp, columns),
        out_shape=[
            jax.ShapeDtypeStruct((depth // (1 if m < tp - 1 else 2), columns), weight.dtype)
            for m in range(tp)
        ],
        in_specs=[HBM_SPEC],
        out_specs=[VMEM_SPEC] * tp,
        scratch_shapes=[pltpu.SemaphoreType.DMA((tp,))],
        compiler_params=pltpu.CompilerParams(vmem_limit_bytes=8 * MIB),
        name="pack_weight",
    )(pltpu.with_memory_space_constraint(weight, pltpu.HBM))


def place_chunk(chunk, owner, layout_ref, k_all, v_all):
    half = chunk.shape[1] // 2
    for b in range(2):
        first = pl.multiple_of(layout_ref[owner * 2 + b] * half, half)
        k_all[pl.ds(first, half), :] = chunk[0, b * half : (b + 1) * half, :]
        for i in range(0, half, HEAD_DIM):
            columns = pl.ds(pl.multiple_of(first + i, HEAD_DIM), HEAD_DIM)
            v_all[:HEAD_DIM, columns] = chunk[1, b * half + i : b * half + i + HEAD_DIM, :]


def owner_of(s, t, spread):
    me = lax.axis_index("ctx")
    return (me // spread ^ s) * spread + (me % spread + spread - t) % spread


def sort_kernel(sources, spread, layout_ref, *refs):
    chunks, (k_all, v_all) = refs[:-2], refs[-2:]
    for chunk, (s, t) in zip(chunks, sources):
        place_chunk(chunk, owner_of(s, t, spread), layout_ref, k_all, v_all)
    half = chunks[0].shape[1] // 2
    total = layout_ref.shape[0] * half
    k_all[total:, :] = jnp.zeros((half, HEAD_DIM), k_all.dtype)
    v_all[:HEAD_DIM, total:] = jnp.zeros((HEAD_DIM, half), v_all.dtype)
    v_all[HEAD_DIM:, :] = jnp.ones((ONES, total + half), v_all.dtype)


def sort(layout, chunks, sources, spread):
    rows = chunks[0].shape[1]
    long = layout.shape[0] * (rows // 2) + rows // 2
    return pl.pallas_call(
        functools.partial(sort_kernel, sources, spread),
        out_shape=[
            jax.ShapeDtypeStruct((long, HEAD_DIM), jnp.bfloat16),
            jax.ShapeDtypeStruct((HEAD_DIM + ONES, long), jnp.bfloat16),
        ],
        in_specs=[SMEM_SPEC] + [VMEM_SPEC] * len(chunks),
        out_specs=[VMEM_SPEC] * 2,
        compiler_params=pltpu.CompilerParams(vmem_limit_bytes=24 * MIB),
        name="sort",
    )(layout, *chunks)


def attention_kernel(place, places, spread, sources, layout_ref, table_ref, bounds_ref, q_ref, *refs):
    refs, (scores, peaks, tops, summed) = refs[:-4], refs[-4:]
    late = refs[2:-3] if len(refs) != 3 else ()
    if late:
        out_ref, k_all, v_all = refs[-3:]
    else:
        k_all, v_all, out_ref = refs
    rows = q_ref.shape[0]
    half = rows // 2
    width = half
    factor = math.log2(math.e) / math.sqrt(HEAD_DIM)

    for chunk, (s, t) in zip(late, sources):
        place_chunk(chunk, owner_of(s, t, spread), layout_ref, k_all, v_all)

    blocks = [table_ref[4 * place + 2 * b] for b in range(2)]
    lows = [table_ref[4 * place + 2 * b + 1] for b in range(2)]
    counts = [blocks[b] - lows[b] + 1 for b in range(2)]
    items = counts[0] + counts[1]
    key_row = lax.broadcasted_iota(jnp.int32, (width, half), 0)
    tops[...] = jnp.full(tops.shape, NEG, jnp.float32)
    summed[...] = jnp.zeros(summed.shape, jnp.float32)

    def where_of(item):
        late = jnp.logical_and(item >= counts[0], item < items).astype(jnp.int32)
        low = jnp.where(late == 1, lows[1], lows[0])
        step = jnp.where(item < items, item - late * counts[0], 0)
        base = pl.multiple_of((low + step) * half, half)
        return late, base

    def score(item, slot):
        late, base = where_of(item)
        raw = lax.dot_general(
            k_all[pl.ds(base, width), :],
            q_ref[pl.ds(pl.multiple_of(late * half, half), half), :],
            (((1,), (1,)), ((), ())),
            preferred_element_type=jnp.float32,
        )
        row = 2 * place + late
        start = bounds_ref[pl.ds(row, 1), :] - jnp.where(item < items, base, -(1 << 30))
        span = bounds_ref[pl.ds(2 * places + row, 1), :].astype(jnp.uint32)
        masked = jnp.where((key_row - start).astype(jnp.uint32) <= span, raw, NEG)
        scores[slot] = masked
        peaks[slot] = jnp.max(masked, axis=0, keepdims=True)

    def absorb(item, slot):
        late, base = where_of(item)
        top = tops[late]
        new_top = jnp.maximum(top, peaks[slot])
        weights = jnp.exp2((scores[slot] - new_top) * factor)
        scale = jnp.exp2((top - new_top) * factor)
        tops[late] = new_top
        summed[late] = summed[late] * scale + jnp.dot(
            v_all[:, pl.ds(base, width)],
            weights.astype(jnp.bfloat16),
            preferred_element_type=jnp.float32,
        )

    for j in range(AHEAD):
        score(j, j)

    def batch(i, carry):
        for j in range(UNROLL):
            score(UNROLL * i + j + AHEAD, (j + AHEAD) % SLOTS)
            absorb(UNROLL * i + j, j % SLOTS)
        return carry

    lax.fori_loop(0, (items + UNROLL - 1) // UNROLL, batch, 0)

    log_rows = []
    for b in range(2):
        sums = summed[b, HEAD_DIM : HEAD_DIM + 1, :]
        mean = summed[b, :HEAD_DIM, :] / sums
        out_ref[b * half : (b + 1) * half, :] = mean.T.astype(jnp.bfloat16)
        logs = tops[b] * (1.0 / math.sqrt(HEAD_DIM)) + jnp.log(sums)
        log_rows += [logs[:, i : i + HEAD_DIM] for i in range(0, half, HEAD_DIM)]
    left = jnp.concatenate(log_rows, axis=0)
    split = []
    for _ in range(3):
        piece = left.astype(jnp.bfloat16).astype(jnp.float32)
        split.append(piece)
        left = left - piece
    split.append(jnp.zeros((LOG_ROWS - 3 * len(log_rows), HEAD_DIM), jnp.float32))
    out_ref[pl.ds(rows, LOG_ROWS), :] = jnp.concatenate(split, axis=0).astype(jnp.bfloat16)


def attend(layout, table, bounds, query, whole, late, sources, place, places, spread):
    rows = query.shape[0]
    half = rows // 2
    out_shape = [jax.ShapeDtypeStruct((rows + LOG_ROWS, HEAD_DIM), jnp.bfloat16)]
    if late:
        out_shape += [jax.ShapeDtypeStruct(x.shape, x.dtype) for x in whole]
    return pl.pallas_call(
        functools.partial(attention_kernel, place, places, spread, sources),
        out_shape=out_shape,
        in_specs=[SMEM_SPEC] * 2 + [VMEM_SPEC] * (4 + len(late)),
        out_specs=[VMEM_SPEC] * len(out_shape),
        input_output_aliases={4: 1, 5: 2} if late else {},
        scratch_shapes=[
            pltpu.VMEM((SLOTS, half, half), jnp.float32),
            pltpu.VMEM((SLOTS, 1, half), jnp.float32),
            pltpu.VMEM((2, 1, half), jnp.float32),
            pltpu.VMEM((2, HEAD_DIM + ONES, half), jnp.float32),
        ],
        compiler_params=pltpu.CompilerParams(vmem_limit_bytes=24 * MIB),
    )(layout, table, bounds, query, *whole, *late)


def weight_rows(w_refs, m, z, side, s, pair):
    head = z ^ s
    count = 2 * HEAD_DIM if pair else HEAD_DIM
    if m < len(w_refs) - 2:
        first = (head // 2) * 2 if pair else head
        return w_refs[m][pl.ds(pl.multiple_of(first * HEAD_DIM, count), count), :]
    rows = pl.ds(0 if pair else pl.multiple_of((head % 2) * HEAD_DIM, HEAD_DIM), count)
    near, far = w_refs[-2:]
    return jnp.where(head // 2 == side, near[rows, :], far[rows, :])


def lone_terms(parts, w_refs, tp, z, side, s):
    total = None
    for m in range(0, tp, 2):
        left = jnp.concatenate([parts[m], parts[m + 1]], axis=1)
        right = jnp.concatenate(
            [weight_rows(w_refs, m + i, z, side, s, False) for i in range(2)], axis=0
        )
        term = jnp.dot(left, right, preferred_element_type=jnp.float32)
        total = term if total is None else total + term
    return total


def early_kernel(spread, tp, *refs):
    parts, w_refs, out_ref = refs[: 3 * tp], refs[3 * tp : -1], refs[-1]
    rows = out_ref.shape[0]
    me = lax.axis_index("ctx")
    z, side = me // spread, me % 2
    total = lone_terms([parts[2 * tp + m][:rows, :] for m in range(tp)], w_refs, tp, z, side, LONE)
    turn = z % 2 == 1
    for m in range(tp):
        here, there = parts[m][:rows, :], parts[tp + m][:rows, :]
        left = jnp.concatenate(
            [jnp.where(turn, there, here), jnp.where(turn, here, there)], axis=1
        )
        right = weight_rows(w_refs, m, z, side, 0, True)
        total = total + jnp.dot(left, right, preferred_element_type=jnp.float32)
    out_ref[...] = total


def late_kernel(places, spread, tp, *refs):
    parts, logs_in, w_refs = refs[:tp], refs[tp : tp + places - 1], refs[tp + places - 1 :]
    w_refs, (early_ref, out_ref, log_ref) = w_refs[:-3], refs[-3:]
    rows = out_ref.shape[0]
    me = lax.axis_index("ctx")
    z, side = me // spread, me % 2
    term = lone_terms([part[:rows, :] for part in parts], w_refs, tp, z, side, LAST)
    out_ref[...] = (early_ref[...] + term).astype(out_ref.dtype)
    count = rows // HEAD_DIM
    logs = {}
    for s, part in zip((0, 1, LONE, LAST), (*logs_in, parts[0])):
        tail = part[pl.ds(rows, LOG_ROWS), :].astype(jnp.float32)
        logs[s] = tail[:count] + tail[count : 2 * count] + tail[2 * count : 3 * count]
    for head in range(places):
        mine = logs[0]
        for s in range(1, places):
            mine = jnp.where(z ^ s == head, logs[s], mine)
        for i in range(count):
            log_ref[head : head + 1, i * HEAD_DIM : (i + 1) * HEAD_DIM] = mine[i : i + 1, :]


def project(groups, weights, places, spread, tp):
    rows = groups[0][0].shape[0] - LOG_ROWS
    columns = weights[0].shape[1]
    params = pltpu.CompilerParams(vmem_limit_bytes=16 * MIB)
    early_parts = [groups[m][s] for s in (0, 1, LONE) for m in range(tp)]
    early = pl.pallas_call(
        functools.partial(early_kernel, spread, tp),
        out_shape=jax.ShapeDtypeStruct((rows, columns), jnp.float32),
        in_specs=[VMEM_SPEC] * (len(early_parts) + len(weights)),
        out_specs=VMEM_SPEC,
        compiler_params=params,
        name="early",
    )(*early_parts, *weights)
    late_parts = [groups[m][LAST] for m in range(tp)] + [groups[0][s] for s in (0, 1, LONE)]
    return pl.pallas_call(
        functools.partial(late_kernel, places, spread, tp),
        out_shape=[
            jax.ShapeDtypeStruct((rows, columns), jnp.bfloat16),
            jax.ShapeDtypeStruct((places, rows), jnp.float32),
        ],
        in_specs=[VMEM_SPEC] * (len(late_parts) + len(weights) + 1),
        out_specs=[VMEM_SPEC] * 2,
        compiler_params=params,
        name="late",
    )(*late_parts, *weights, early)


def local(ctx, tp, queries, keys, values, out_weight, doc_lengths, layout):
    places = queries.shape[1] // HEAD_DIM
    spread = ctx // places
    assert places == 4 and tp == 4 and spread % 2 == 0

    def move(array, axis, target):
        count = ctx if axis == "ctx" else tp
        return lax.ppermute(array, axis, [(i, target(i)) for i in range(count)])

    def over_places(array, s):
        return move(array, "ctx", lambda i: ((i // spread) ^ s) * spread + i % spread)

    def over_spread(array, t):
        return move(array, "ctx", lambda i: i // spread * spread + (i % spread + t) % spread)

    def over_tp(array, m):
        return move(array, "tp", lambda i: i ^ m)

    packed = pack(keys, values, queries, places, spread)
    kv, q = packed[:places], packed[places:]
    q = [q[0]] + [over_places(q[s], s) for s in range(1, places)]
    chunks = {}
    for s in range(places):
        chunks[s, 0] = over_places(kv[s], s) if s else kv[0]
        for t in range(1, spread):
            chunks[s, t] = over_spread(chunks[s, 0], t)

    packed_weight = pack_weight(out_weight, tp)
    weights = [packed_weight[0]] + [over_tp(packed_weight[m], m) for m in range(1, tp)]
    weights.append(move(weights[-1], "ctx", lambda i: i ^ 1))

    table, bounds = plan(layout, doc_lengths, places, spread, keys.shape[0] // 2)
    late = [(LAST, t) for t in range(1, spread)]
    soon = [source for source in chunks if source not in late]
    whole = sort(layout, [chunks[source] for source in soon], soon, spread)
    heads = [None] * places
    for s in ATTEND_ORDER:
        extra = [chunks[source] for source in late]
        message, *rest = attend(layout, table, bounds, q[s], whole, extra, late, s, places, spread)
        whole, late = rest or whole, []
        heads[s] = over_places(message, s) if s else message

    groups = [heads]
    groups.append([over_tp(heads[s], 1) for s in range(places)])
    groups.append([over_tp(heads[s], 2) for s in range(places)])
    groups.append([over_tp(groups[2][s], 1) for s in range(places)])
    return project(groups, weights, places, spread, tp)


def solution(mesh):
    placed = (P("ctx", "tp"), P("ctx", "tp"), P("ctx", "tp"), P("tp", None), P(), P())
    return jax.shard_map(
        functools.partial(local, mesh.shape["ctx"], mesh.shape["tp"]),
        mesh=mesh,
        in_specs=placed,
        out_specs=(P("ctx", "tp"), P("tp", "ctx")),
        check_vma=False,
    )
```
